32 devices in a mesh: seq: 8 (over z, y), ch: 4 (over x, core).
Axes of the slice: x: 2, y: 2, z: 4, core: 2. Of those that a mesh axis runs over, the one named last changes fastest.
Arguments:
- signal: float32 [1, 65536, 1024], P(None, 'seq', 'ch'), may hold values from -6 to 6
- spectrum: float32 [2, 256, 256, 1024], P(None, 'seq', None, 'ch'), may hold values from -6 to 6
- channel_mode: int32 [1024], P('ch'), may hold values 0 or 1
- skip_gain: float32 [1024], P('ch'), may hold values from -4 to 4
- out_weight: bfloat16 [1024, 1024], P('ch'), may hold values from -0.1875 to 0.1875
Outputs:
- projected: float32 [1, 65536, 1024], P(None, 'seq', 'ch')
The draws below stay inside these ranges and needn't reach their ends.
Inputs may be any that keep to these rules, and one draw needn't show every extreme that they name: `channel_mode`: 1 marks a channel whose 65536 positions are one sequence, 0 a channel whose positions form a 256 x 256 image.
All inputs are finite; a program needn't handle non-finite values. No bound on the sum of `channel_mode` on one device may be relied on, other than what follows from the above.
Results may differ from the reference program's by a relative error of at most 0.017.
Values may be sent and summed in bfloat16 or wider, within the bound.
No kernel may reach another device: no remote copies, remote signals or barrier semaphores. Data moves between devices by JAX's collectives and lax.ppermute only.
A program may use at most 192 MiB of HBM per device.

```python
import jax
import jax.numpy as jnp
from jax import lax

BATCH = 1
WIDTH = 1024
ROWS = 256
COLUMNS = 256
LENGTH = 65536
N_CH = 4


def place_ends(values, key, low, high):
    place = [jax.random.randint(jax.random.fold_in(key, axis), (), 0, length) for axis, length in enumerate(values.shape)]
    main_axis = values.shape.index(max(values.shape))
    neighbour = place[:main_axis] + [(place[main_axis] + 1) % values.shape[main_axis]] + place[main_axis + 1:]
    return values.at[tuple(place)].set(low).at[tuple(neighbour)].set(high)


def levels(rng, extent, shards, smallest, largest):
    def one(position, shards_of):
        steps = jax.random.uniform(jax.random.fold_in(jax.random.fold_in(rng, 6), position), (shards_of,), jnp.float32, smallest / len(shards), largest / len(shards))
        return jnp.repeat(jnp.exp(steps), extent[position] // shards_of).reshape((-1,) + (1,) * (len(extent) - position - 1))

    level = one(*shards[0])
    for cut in shards[1:]:
        level = level * one(*cut)
    return level


def centred(stream_key, dims, width, limit, cuts=(), dtype=jnp.bfloat16):
    drawn = width * jax.random.normal(stream_key, dims, jnp.float32)
    if cuts:
        drawn = drawn * levels(stream_key, dims, cuts, -0.22, 0.18)
    return jnp.clip(drawn, -limit, limit).astype(dtype)


def setup_inputs(seed: int = 0) -> dict:
    splits = jax.random.split(jax.random.key(seed), 6)
    signal = centred(splits[0], (BATCH, LENGTH, WIDTH), 1.0, 6.0, ((1, 8), (2, 4)), jnp.float32)
    spectrum = centred(splits[1], (2, ROWS, COLUMNS, WIDTH), 0.7071, 6.0, ((1, 8), (3, 4)), jnp.float32)
    channel_mode = place_ends((jax.random.randint(splits[2], (WIDTH,), 0, 2) < 1).astype(jnp.int32), jax.random.fold_in(splits[2], 1), 0, 1)
    skip_gain = centred(splits[3], (WIDTH,), 1.0, 4.0, ((0, 4),), jnp.float32)
    out_weight = centred(splits[4], (WIDTH, WIDTH), WIDTH ** -0.5, 0.1875, ((0, 4),))
    return {"signal": signal, "spectrum": spectrum, "channel_mode": channel_mode, "skip_gain": skip_gain, "out_weight": out_weight}


def convolve_block(packed):
    signal_block, spectrum_block, mode_block, gain_block = packed
    series = jnp.transpose(signal_block, (0, 2, 1))
    filters = lax.complex(spectrum_block[0], spectrum_block[1])
    filters = jnp.transpose(filters, (2, 0, 1))
    linear_filter = jnp.transpose(filters, (0, 2, 1)).reshape(filters.shape[0], LENGTH)
    linear = jnp.real(jnp.fft.ifft(jnp.fft.fft(series, axis=-1) * linear_filter[None], axis=-1))
    images = series.reshape(series.shape[0], series.shape[1], ROWS, COLUMNS)
    planar = jnp.real(jnp.fft.ifft2(jnp.fft.fft2(images, axes=(-2, -1)) * filters[None], axes=(-2, -1)))
    planar = planar.reshape(series.shape)
    convolved = jnp.where(mode_block[None, :, None] == 1, linear, planar)
    hidden = convolved + gain_block[None, :, None] * series
    return jnp.transpose(hidden, (0, 2, 1)).astype(jnp.float32)


def reference(signal, spectrum, channel_mode, skip_gain, out_weight):
    block_width = WIDTH // N_CH
    signal_parts = jnp.moveaxis(signal.reshape(BATCH, LENGTH, N_CH, block_width), 2, 0)
    spectrum_parts = jnp.moveaxis(spectrum.reshape(2, ROWS, COLUMNS, N_CH, block_width), 3, 0)
    mode_parts = channel_mode.reshape(N_CH, block_width)
    gain_parts = skip_gain.reshape(N_CH, block_width)
    hidden_parts = lax.map(convolve_block, (signal_parts, spectrum_parts, mode_parts, gain_parts))
    hidden_parts = hidden_parts.astype(jnp.bfloat16)
    weight_parts = out_weight.reshape(N_CH, block_width, WIDTH)

    def add_block(running, packed):
        features, weights = packed
        partial_value = jnp.dot(features.reshape(BATCH * LENGTH, block_width), weights, preferred_element_type=jnp.float32)
        partial_value = lax.optimization_barrier(partial_value.astype(jnp.bfloat16))
        return running + partial_value.astype(jnp.float32), jnp.zeros((), jnp.float32)

    initial = jnp.zeros((BATCH * LENGTH, WIDTH), jnp.float32)
    total, unused = lax.scan(add_block, initial, (hidden_parts, weight_parts))
    return total.reshape(BATCH, LENGTH, WIDTH)
```

```python
import math

import jax
import jax.numpy as jnp
from jax import lax
from jax.experimental import pallas as pl
from jax.experimental.pallas import tpu as pltpu
from jax.sharding import PartitionSpec as P

CHUNKS = 4


def phase_table(row_index, col_index, period):
    product = row_index[:, None] * col_index[None, :] % period
    angles = product.astype(jnp.float32) * (2.0 * math.pi / period)
    return (jnp.cos(angles), jnp.sin(angles))


def square_table(length):
    counter = jnp.arange(length, dtype=jnp.int32)
    return phase_table(counter, counter, length)


def block_matrix(cosine, sine):
    top = jnp.concatenate([cosine, -sine], axis=1)
    bottom = jnp.concatenate([sine, cosine], axis=1)
    return jnp.concatenate([top, bottom], axis=0)


def conv_kernel(mode, *refs):
    first, forward, backward, last, twist, out = refs[-6:]
    pieces = (len(refs) - 6) // 2
    signal, spectrum = refs[:pieces], refs[pieces : 2 * pieces]
    rows, cols = out.shape[1:]
    which = mode[pl.program_id(0)]
    image = jnp.concatenate([piece[0] for piece in signal], axis=0)
    spread = jnp.dot(first[...], image, preferred_element_type=jnp.float32)
    real, imag = spread[:rows], spread[rows:]
    cosine, sine = twist[which, 0], twist[which, 1]
    turned = jnp.concatenate(
        [
            (real * cosine + imag * sine).astype(jnp.bfloat16),
            (imag * cosine - real * sine).astype(jnp.bfloat16),
        ],
        axis=1,
    )
    full = jnp.dot(turned, forward[...], preferred_element_type=jnp.float32)
    real, imag = full[:, :cols], full[:, cols:]
    weight_real = jnp.concatenate([piece[0, 0] for piece in spectrum], axis=0).astype(jnp.float32)
    weight_imag = jnp.concatenate([piece[0, 1] for piece in spectrum], axis=0).astype(jnp.float32)
    filtered = jnp.concatenate(
        [
            (real * weight_real - imag * weight_imag).astype(jnp.bfloat16),
            (real * weight_imag + imag * weight_real).astype(jnp.bfloat16),
        ],
        axis=1,
    )
    half = jnp.dot(filtered, backward[...], preferred_element_type=jnp.float32)
    real, imag = half[:, :cols], half[:, cols:]
    turned = jnp.concatenate(
        [
            (real * cosine - imag * sine).astype(jnp.bfloat16),
            (real * sine + imag * cosine).astype(jnp.bfloat16),
        ],
        axis=0,
    )
    out[0] = jnp.dot(last[...], turned, preferred_element_type=jnp.float32).astype(out.dtype)


def convolve(modes, signal, spectrum, tables):
    groups = len(signal)
    count, local, cols = signal[0].shape
    rows = groups * local
    whole = lambda table: pl.BlockSpec(table.shape, lambda i, m: (0,) * table.ndim)
    return pl.pallas_call(
        conv_kernel,
        grid_spec=pltpu.PrefetchScalarGridSpec(
            num_scalar_prefetch=1,
            grid=(count,),
            in_specs=[pl.BlockSpec((1, local, cols), lambda i, m: (i, 0, 0))] * groups
            + [pl.BlockSpec((1, 2, local, cols), lambda i, m: (i, 0, 0, 0))] * groups
            + [whole(table) for table in tables],
            out_specs=pl.BlockSpec((1, rows, cols), lambda i, m: (i, 0, 0)),
        ),
        out_shape=jax.ShapeDtypeStruct((count, rows, cols), jnp.bfloat16),
        cost_estimate=pl.CostEstimate(
            flops=24 * count * rows * cols * 256, transcendentals=0, bytes_accessed=8 * count * rows * cols
        ),
        name="conv",
    )(modes, *signal, *spectrum, *tables)


def per_device(signal, spectrum, channel_mode, skip_gain, out_weight):
    groups = lax.axis_size("seq")
    blocks = lax.axis_size("ch")
    position = lax.axis_index("seq")
    local, cols, owned = spectrum.shape[1:]
    rows = local * groups
    shared = owned // groups
    chunks = CHUNKS
    while shared % chunks:
        chunks //= 2
    count = shared // chunks
    width = out_weight.shape[1]
    sub = local // blocks

    weights = lax.all_gather(out_weight, "ch").reshape(blocks, groups, chunks, count, width)
    own_modes = lax.dynamic_slice_in_dim(channel_mode, position * shared, shared)

    held = (position ^ jnp.arange(groups, dtype=jnp.int32))[:, None] * local
    held = (held + jnp.arange(local, dtype=jnp.int32)[None, :]).reshape(rows)
    natural = jnp.arange(rows, dtype=jnp.int32)
    near_cos, near_sin = phase_table(held, held, rows)
    far_cos, far_sin = phase_table(natural, held, rows)
    col_cos, col_sin = square_table(cols)
    twist = phase_table(held, jnp.arange(cols, dtype=jnp.int32), rows * cols)
    flat = jnp.stack([jnp.ones_like(twist[0]), jnp.zeros_like(twist[0])])
    tables = (
        jnp.concatenate([near_cos, -near_sin], axis=0).astype(jnp.bfloat16),
        block_matrix(col_cos, col_sin).astype(jnp.bfloat16),
        block_matrix(col_cos, -col_sin).astype(jnp.bfloat16),
        (jnp.concatenate([far_cos, -far_sin], axis=1) / (rows * cols)).astype(jnp.bfloat16),
        jnp.stack([flat, jnp.stack(twist)]),
    )
    tables = lax.optimization_barrier(tables)

    gained = jnp.concatenate([spectrum[:1] + skip_gain, spectrum[1:]], axis=0)
    sent_signal = jnp.transpose(signal.reshape(local, cols, owned).astype(jnp.bfloat16), (2, 0, 1))
    sent_signal = sent_signal.reshape(groups, chunks, count, local, cols)
    sent_filter = jnp.transpose(gained.astype(jnp.bfloat16), (3, 0, 1, 2))
    sent_filter = sent_filter.reshape(groups, chunks, count, 2, local, cols)

    sent_signal = lax.optimization_barrier(sent_signal)
    sent_filter = lax.optimization_barrier(sent_filter)

    def swap(sent, chunk):
        pieces = []
        for step in range(groups):
            start = (position ^ step, chunk) + (0,) * (sent.ndim - 2)
            piece = lax.dynamic_slice(sent, start, (1, 1) + sent.shape[2:])[0, 0]
            if step:
                piece = lax.ppermute(piece, "seq", [(s, s ^ step) for s in range(groups)])
            pieces.append(piece)
        return pieces

    arrived = [(swap(sent_signal, k), swap(sent_filter, k)) for k in range(chunks)]
    total = None
    for k in range(chunks):
        image, spectra = arrived[k]
        result = convolve(own_modes[k * count : (k + 1) * count], image, spectra, tables)
        result = jnp.transpose(result.reshape(count, groups * blocks, sub, cols), (1, 0, 2, 3))
        hidden = lax.all_to_all(result, ("seq", "ch"), split_axis=0, concat_axis=0, tiled=True)
        hidden = hidden.reshape(groups, blocks, count, sub, cols)
        part = jnp.einsum(
            "sciae,csij->aej", hidden, weights[:, :, k], preferred_element_type=jnp.float32
        )
        total = part if total is None else total + part
    outgoing = total.astype(jnp.bfloat16).reshape(sub * cols, blocks, width // blocks)
    outgoing = jnp.transpose(outgoing, (1, 0, 2))
    final = lax.all_to_all(outgoing, "ch", split_axis=0, concat_axis=0, tiled=True)
    return final.reshape(1, local * cols, width // blocks).astype(jnp.float32)


def solution(mesh):
    placed = (P(None, "seq", "ch"), P(None, "seq", None, "ch"), P("ch"), P("ch"), P("ch", None))
    return jax.shard_map(
        per_device, mesh=mesh, in_specs=placed, out_specs=P(None, "seq", "ch"), check_vma=False
    )
```
